32 devices in a mesh: frame: 8 (over z, core), mp: 2 (over x), dp: 2 (over y).
Axes of the slice: x: 2, y: 2, z: 4, core: 2. Of those that a mesh axis runs over, the one named last changes fastest.
Arguments:
- tokens: bfloat16 [4, 8, 160, 5120], P('dp', 'frame', None, 'mp'), may hold values from -30 to 30
- token_mask: int32 [4, 8, 160], P('dp', 'frame'), may hold values 0 or 1
- mask_embed: bfloat16 [5120], P('mp'), may hold values from -6 to 6
- w_qkv: bfloat16 [5120, 3, 3072], P('frame', None, 'mp'), may hold values from -0.078125 to 0.078125
- w_out: bfloat16 [3072, 5120], P('mp'), may hold values from -0.109375 to 0.109375
- action_idx: int32 [4, 8], P('dp', 'frame'), may hold values from 0 to 7
- codebook: float32 [8, 32], replicated, may hold values from -6 to 6
- act_proj: float32 [32, 5120], P(None, 'mp'), may hold values from -1 to 1
- cotangent: bfloat16 [4, 8, 160, 5120], P('dp', 'frame', None, 'mp'), may hold values from -6 to 6
Outputs:
- next_state: bfloat16 [4, 8, 160, 5120], P('dp', 'frame', None, 'mp')
- grad_proj: float32 [32, 5120], P(None, 'mp')
The draws below stay inside these ranges and needn't reach their ends.
All inputs are finite; a program needn't handle non-finite values. No bound on the sum of `token_mask` on one device may be relied on, other than what follows from the above.
Results may differ from the reference program's by a relative error of at most 0.0098.
Values may be sent and summed in bfloat16 or wider, within the bound.
A program may use at most 128 MiB of HBM per device.

```python
import jax
import jax.numpy as jnp
from jax import lax

D = 5120
HEADS = 24
HS = 128
CODES = 8
D_ACT = 32
P_SIZE = 160
CLIPS = 4
FRAMES = 8


def draw_tokens(key, part):
    shape = (CLIPS, FRAMES, P_SIZE, D)
    return jax.random.truncated_normal(key, -6.0, 6.0, shape, jnp.float32).astype(jnp.bfloat16)


def touch_ends(result, rng, low, largest):
    longest = result.shape.index(max(result.shape))
    spots = []
    for shift in (0, 1):
        where = [jax.random.randint(jax.random.fold_in(rng, axis), (), 0, length) for axis, length in enumerate(result.shape)]
        where[longest] = (where[longest] + shift) % result.shape[longest]
        spots.append(tuple(where))
    return result.at[spots[0]].set(low).at[spots[1]].set(largest)


def block_scale(key, shape, cuts, smallest, high):
    factor_of, own = 1.0, jax.random.fold_in(key, 6)
    for axis_at, parts in cuts:
        heights = jnp.exp(jax.random.uniform(jax.random.fold_in(own, axis_at), (parts,), jnp.float32, smallest / len(cuts), high / len(cuts)))
        factor_of = factor_of * jnp.repeat(heights, shape[axis_at] // parts).reshape([-1 if axis == axis_at else 1 for axis in range(len(shape))])
    return factor_of


def centred(key, dims, scale, bound, cuts=(), dtype=jnp.bfloat16):
    factor_of = block_scale(key, dims, cuts, -0.22, 0.18) if cuts else 1.0
    array = jax.random.normal(key, dims, jnp.float32) * scale * factor_of
    return jnp.minimum(jnp.maximum(array, -bound), bound).astype(dtype)


def setup_inputs(seed: int = 0) -> dict:
    splits = jax.random.split(jax.random.key(seed), 10)
    tokens = draw_tokens(jax.random.fold_in(splits[9], 71), 0)
    token_mask = touch_ends((jax.random.randint(splits[1], (CLIPS, FRAMES, P_SIZE), 0, 2) < 1).astype(jnp.int32), jax.random.fold_in(splits[1], 1), 0, 1)
    mask_embed = centred(splits[2], (D,), 1.0, 6.0, ((0, 2),))
    w_qkv = centred(splits[3], (D, 3, HEADS * HS), D ** -0.5, 0.078125, ((0, 8), (2, 2)))
    w_out = centred(splits[4], (HEADS * HS, D), (HEADS * HS) ** -0.5, 0.109375, ((0, 2),))
    action_idx = touch_ends(jax.random.randint(splits[5], (CLIPS, FRAMES), 0, CODES), jax.random.fold_in(splits[5], 1), 0, CODES - 1).astype(jnp.int32)
    codebook = centred(splits[6], (CODES, D_ACT), 1.0, 6.0, (), jnp.float32)
    act_proj = centred(splits[7], (D_ACT, D), D_ACT ** -0.5, 1.0, ((1, 2),), jnp.float32)
    cotangent = centred(splits[8], (CLIPS, FRAMES, P_SIZE, D), 1.0, 6.0, ((0, 2), (1, 8), (3, 2)))
    return dict(tokens=tokens, token_mask=token_mask, mask_embed=mask_embed, w_qkv=w_qkv, w_out=w_out, action_idx=action_idx, codebook=codebook, act_proj=act_proj, cotangent=cotangent)


def reference(tokens, token_mask, mask_embed, w_qkv, w_out, action_idx, codebook, act_proj, cotangent):
    xin = jnp.where(token_mask[..., None] == 1, mask_embed, tokens)
    width_heads = HEADS * HS
    flat = xin.reshape(-1, D)
    qkv = jnp.dot(flat, w_qkv.reshape(D, 3 * width_heads), preferred_element_type=jnp.float32).astype(jnp.bfloat16)
    qkv = qkv.reshape(CLIPS, FRAMES, P_SIZE, 3, HEADS, HS)
    query = qkv[:, :, :, 0].astype(jnp.float32)
    keys = qkv[:, :, :, 1].astype(jnp.float32)
    values = qkv[:, :, :, 2].astype(jnp.float32)
    scores = jnp.einsum('cfphd,cuphd->cfphu', query, keys, precision=lax.Precision.HIGHEST) / jnp.sqrt(jnp.float32(HS))
    causal = (jnp.arange(FRAMES)[:, None] >= jnp.arange(FRAMES)[None, :])[None, :, None, None, :]
    peak = lax.optimization_barrier(jnp.max(jnp.where(causal, scores, -jnp.inf), axis=-1))
    weights = jnp.where(causal, jnp.exp(scores - peak[..., None]), 0.0)
    total = lax.optimization_barrier(jnp.sum(weights, axis=-1))
    accum = jnp.einsum('cfphu,cuphd->cfphd', weights, values, precision=lax.Precision.HIGHEST)
    attn = (accum / total[..., None]).astype(jnp.bfloat16).reshape(-1, width_heads)
    mixed = jnp.dot(attn, w_out, preferred_element_type=jnp.float32).reshape(CLIPS, FRAMES, P_SIZE, D)
    codevec = codebook[action_idx].reshape(-1, D_ACT)
    gate = jnp.dot(codevec, act_proj, precision=lax.Precision.HIGHEST).reshape(CLIPS, FRAMES, 1, D)
    next_state = (xin.astype(jnp.float32) + gate * mixed).astype(jnp.bfloat16)
    dgate = lax.optimization_barrier(jnp.sum(cotangent.astype(jnp.float32) * mixed, axis=2)).reshape(-1, D)
    grad_proj = jnp.dot(codevec.T, dgate, precision=lax.Precision.HIGHEST)
    return (next_state, grad_proj)
```

```python
import functools
import math

import jax
import jax.numpy as jnp
from jax import lax
from jax.experimental import pallas as pl
from jax.experimental.pallas import tpu as pltpu
from jax.sharding import PartitionSpec as P

HS = 128


def attend_kernel(frames, q_ref, k_ref, v_ref, o_ref):
    scale = 1.0 / math.sqrt(HS)
    for t in range(frames):
        q = q_ref[t].astype(jnp.float32) * scale
        scores = [
            jnp.sum(q * k_ref[u].astype(jnp.float32), axis=-1, keepdims=True) for u in range(t + 1)
        ]
        peak = functools.reduce(jnp.maximum, scores)
        weights = [jnp.exp(s - peak) for s in scores]
        total = functools.reduce(jnp.add, weights)
        accum = functools.reduce(
            jnp.add, [w * v_ref[u].astype(jnp.float32) for u, w in enumerate(weights)]
        )
        o_ref[t] = (accum / total).astype(o_ref.dtype)


def attend(qkv, frames, heads_width):
    rows = qkv.shape[1]
    heads = heads_width // HS
    spec = lambda part: pl.BlockSpec((frames, rows, HS), lambda h, part=part: (0, 0, part * heads + h))
    return pl.pallas_call(
        functools.partial(attend_kernel, frames),
        grid=(heads,),
        in_specs=[spec(0), spec(1), spec(2)],
        out_specs=spec(0),
        out_shape=jax.ShapeDtypeStruct((frames, rows, heads_width), jnp.bfloat16),
        cost_estimate=pl.CostEstimate(flops=4 * frames * frames * rows * heads_width,
                                      bytes_accessed=8 * frames * rows * heads_width,
                                      transcendentals=0),
        name="attend",
    )(qkv, qkv, qkv)


def gather_mp(block, size):
    if size != 2:
        return lax.all_gather(block, "mp", axis=block.ndim - 1, tiled=True)
    other = lax.ppermute(block, "mp", [(0, 1), (1, 0)])
    first = lax.axis_index("mp") == 0
    return jnp.concatenate(
        [jnp.where(first, block, other), jnp.where(first, other, block)], axis=-1
    )


def body(mp_size, dp_size, tokens, token_mask, mask_embed, w_qkv, w_out, action_idx, codebook,
         act_proj, cotangent):
    clips, _, spots, width = tokens.shape
    heads_width = w_qkv.shape[2]
    depth = w_qkv.shape[0]
    xin = jnp.where(token_mask[..., None] == 1, mask_embed, tokens)
    share = depth // dp_size
    mine = lax.dynamic_slice_in_dim(
        w_qkv.reshape(depth, 3 * heads_width), lax.axis_index("dp") * share, share, axis=0
    )
    weights = lax.all_gather(mine, ("frame", "dp"), axis=0, tiled=True)
    spread = lax.all_to_all(
        xin.reshape(clips, spots, width), "frame", split_axis=1, concat_axis=0, tiled=True
    )
    frames = spread.shape[0] // clips
    local = spread.shape[1]
    features = gather_mp(spread.reshape(frames * clips * local, width), mp_size)
    qkv = jnp.dot(features, weights, preferred_element_type=jnp.float32).astype(jnp.bfloat16)
    attn = attend(qkv.reshape(frames, clips * local, 3 * heads_width), frames, heads_width)
    back = lax.all_to_all(
        attn.reshape(frames * clips, local, heads_width), "frame", split_axis=0, concat_axis=1,
        tiled=True,
    )
    all_heads = gather_mp(back.reshape(clips * spots, heads_width), mp_size)
    out_block = lax.all_to_all(w_out, "mp", split_axis=1, concat_axis=0, tiled=True)
    mixed_rows = jnp.dot(all_heads, out_block, preferred_element_type=jnp.float32)
    mixed = mixed_rows.reshape(clips, 1, spots, width)
    onehot = (
        action_idx.reshape(clips)[:, None] == jnp.arange(codebook.shape[0])[None, :]
    ).astype(jnp.float32)
    codevec = jnp.dot(onehot, codebook, precision=lax.Precision.HIGHEST)
    gate = jnp.dot(codevec, act_proj, precision=lax.Precision.HIGHEST)
    next_state = (xin.astype(jnp.float32) + gate[:, None, None, :] * mixed).astype(jnp.bfloat16)
    dgate = jnp.sum(cotangent.astype(jnp.float32) * mixed, axis=2).reshape(clips, width)
    codes_all = lax.all_gather(codevec, ("frame", "dp"), axis=0, tiled=True)
    dgate_all = lax.all_gather(dgate, ("frame", "dp"), axis=0, tiled=True)
    grad_proj = jnp.dot(codes_all.T, dgate_all, precision=lax.Precision.HIGHEST)
    return (next_state, grad_proj)


def solution(mesh):
    in_specs = (
        P("dp", "frame", None, "mp"),
        P("dp", "frame", None),
        P("mp"),
        P("frame", None, "mp"),
        P("mp", None),
        P("dp", "frame"),
        P(),
        P(None, "mp"),
        P("dp", "frame", None, "mp"),
    )
    out_specs = (P("dp", "frame", None, "mp"), P(None, "mp"))
    return jax.shard_map(
        functools.partial(body, mesh.shape["mp"], mesh.shape["dp"]),
        mesh=mesh, in_specs=in_specs, out_specs=out_specs, check_vma=False,
    )
```

```python
import functools
import math

import jax
import jax.numpy as jnp
from jax import lax
from jax.experimental import pallas as pl
from jax.experimental.pallas import tpu as pltpu
from jax.sharding import PartitionSpec as P

HS = 128


def attend_kernel(frames, q_ref, k_ref, v_ref, o_ref):
    scale = 1.0 / math.sqrt(HS)
    for t in range(frames):
        q = q_ref[t].astype(jnp.float32) * scale
        scores = [
            jnp.sum(q * k_ref[u].astype(jnp.float32), axis=-1, keepdims=True) for u in range(t + 1)
        ]
        peak = functools.reduce(jnp.maximum, scores)
        weights = [jnp.exp(s - peak) for s in scores]
        total = functools.reduce(jnp.add, weights)
        accum = functools.reduce(
            jnp.add, [w * v_ref[u].astype(jnp.float32) for u, w in enumerate(weights)]
        )
        o_ref[t] = (accum / total).astype(o_ref.dtype)


def attend(qkv, frames, heads_width):
    rows = qkv.shape[1]
    heads = heads_width // HS
    spec = lambda part: pl.BlockSpec((frames, rows, HS), lambda h, part=part: (0, 0, part * heads + h))
    return pl.pallas_call(
        functools.partial(attend_kernel, frames),
        grid=(heads,),
        in_specs=[spec(0), spec(1), spec(2)],
        out_specs=spec(0),
        out_shape=jax.ShapeDtypeStruct((frames, rows, heads_width), jnp.bfloat16),
        cost_estimate=pl.CostEstimate(flops=4 * frames * frames * rows * heads_width,
                                      bytes_accessed=8 * frames * rows * heads_width,
                                      transcendentals=0),
        name="attend",
    )(qkv, qkv, qkv)


def spread_kernel(frames, dps, x_ref, o_ref, send_sem, recv_sem, own_sem):
    count = frames * dps
    me = lax.axis_index("frame") * dps + lax.axis_index("dp")
    barrier = pltpu.get_barrier_semaphore()

    def peer(shift):
        other = lax.rem(me + shift, count)
        return {"frame": other // dps, "dp": lax.rem(other, dps)}

    for shift in range(1, count):
        pl.semaphore_signal(barrier, inc=1, device_id=peer(shift),
                            device_id_type=pl.DeviceIdType.MESH)
    own = pltpu.make_async_copy(x_ref, o_ref.at[me], own_sem)
    own.start()
    pl.semaphore_wait(barrier, count - 1)
    copies = []
    for shift in range(1, count):
        copy = pltpu.make_async_remote_copy(
            src_ref=x_ref, dst_ref=o_ref.at[me], send_sem=send_sem.at[shift],
            recv_sem=recv_sem.at[shift], device_id=peer(shift),
            device_id_type=pl.DeviceIdType.MESH)
        copy.start()
        copies.append(copy)
    own.wait()
    for copy in copies:
        copy.wait()


def spread_terms(terms, frames, dps):
    count = frames * dps
    return pl.pallas_call(
        functools.partial(spread_kernel, frames, dps),
        in_specs=[pl.BlockSpec(memory_space=pltpu.VMEM)],
        out_specs=pl.BlockSpec(memory_space=pltpu.VMEM),
        out_shape=jax.ShapeDtypeStruct((count, *terms.shape), terms.dtype),
        scratch_shapes=[pltpu.SemaphoreType.DMA((count,)), pltpu.SemaphoreType.DMA((count,)),
                        pltpu.SemaphoreType.DMA],
        compiler_params=pltpu.CompilerParams(collective_id=1, has_side_effects=True),
        name="spread_terms",
    )(terms)


def gather_mp(block, size):
    if size != 2:
        return lax.all_gather(block, "mp", axis=block.ndim - 1, tiled=True)
    other = lax.ppermute(block, "mp", [(0, 1), (1, 0)])
    first = lax.axis_index("mp") == 0
    return jnp.concatenate(
        [jnp.where(first, block, other), jnp.where(first, other, block)], axis=-1
    )


def body(mp_size, dp_size, tokens, token_mask, mask_embed, w_qkv, w_out, action_idx, codebook,
         act_proj, cotangent):
    clips, _, spots, width = tokens.shape
    heads_width = w_qkv.shape[2]
    depth = w_qkv.shape[0]
    xin = jnp.where(token_mask[..., None] == 1, mask_embed, tokens)
    share = depth // dp_size
    mine = lax.dynamic_slice_in_dim(
        w_qkv.reshape(depth, 3 * heads_width), lax.axis_index("dp") * share, share, axis=0
    )
    weights = lax.all_gather(mine, ("frame", "dp"), axis=0, tiled=True)
    if mp_size == 2:
        my_mp = lax.axis_index("mp")
        out_mine = lax.dynamic_slice_in_dim(w_out, my_mp * width, width, axis=1)
        out_other = lax.ppermute(
            lax.dynamic_slice_in_dim(w_out, (1 - my_mp) * width, width, axis=1),
            "mp", [(0, 1), (1, 0)])
    spread = lax.all_to_all(
        xin.reshape(clips, spots, width), "frame", split_axis=1, concat_axis=0, tiled=True
    )
    frames = spread.shape[0] // clips
    local = spread.shape[1]
    features = gather_mp(spread.reshape(frames * clips * local, width), mp_size)
    qkv = jnp.dot(features, weights, preferred_element_type=jnp.float32).astype(jnp.bfloat16)
    attn = attend(qkv.reshape(frames, clips * local, 3 * heads_width), frames, heads_width)
    back = lax.all_to_all(
        attn.reshape(frames * clips, local, heads_width), "frame", split_axis=0, concat_axis=1,
        tiled=True,
    )
    heads = back.reshape(clips * spots, heads_width)
    if mp_size == 2:
        other_heads = lax.ppermute(heads, "mp", [(0, 1), (1, 0)])
        mixed_rows = jnp.dot(heads, out_mine, preferred_element_type=jnp.float32) + jnp.dot(
            other_heads, out_other, preferred_element_type=jnp.float32)
    else:
        out_block = lax.all_to_all(w_out, "mp", split_axis=1, concat_axis=0, tiled=True)
        mixed_rows = jnp.dot(gather_mp(heads, mp_size), out_block,
                             preferred_element_type=jnp.float32)
    mixed = mixed_rows.reshape(clips, 1, spots, width)
    onehot = (
        action_idx.reshape(clips)[:, None] == jnp.arange(codebook.shape[0])[None, :]
    ).astype(jnp.float32)
    codevec = jnp.dot(onehot, codebook, precision=lax.Precision.HIGHEST)
    gate = jnp.dot(codevec, act_proj, precision=lax.Precision.HIGHEST)
    next_state = (xin.astype(jnp.float32) + gate[:, None, None, :] * mixed).astype(jnp.bfloat16)
    dgate = jnp.sum(cotangent.astype(jnp.float32) * mixed, axis=2).reshape(clips, width)
    codes = codevec.shape[1]
    padded = jnp.pad(codevec, ((0, 0), (0, -codes % 128)))
    terms = spread_terms(jnp.concatenate([dgate, padded], axis=1), frames, dp_size)
    terms = terms.reshape(frames * dp_size * clips, -1)
    grad_proj = jnp.dot(
        terms[:, width : width + codes].T, terms[:, :width], precision=lax.Precision.HIGHEST)
    return (next_state, grad_proj)


def solution(mesh):
    in_specs = (
        P("dp", "frame", None, "mp"),
        P("dp", "frame", None),
        P("mp"),
        P("frame", None, "mp"),
        P("mp", None),
        P("dp", "frame"),
        P(),
        P(None, "mp"),
        P("dp", "frame", None, "mp"),
    )
    out_specs = (P("dp", "frame", None, "mp"), P(None, "mp"))
    return jax.shard_map(
        functools.partial(body, mesh.shape["mp"], mesh.shape["dp"]),
        mesh=mesh, in_specs=in_specs, out_specs=out_specs, check_vma=False,
    )
```

```python
import functools
import math

import jax
import jax.numpy as jnp
from jax import lax
from jax.experimental import pallas as pl
from jax.experimental.pallas import tpu as pltpu
from jax.sharding import PartitionSpec as P

HS = 128


def attend_kernel(frames, q_ref, k_ref, v_ref, o_ref):
    scale = 1.0 / math.sqrt(HS)
    for t in range(frames):
        q = q_ref[t].astype(jnp.float32) * scale
        scores = [
            jnp.sum(q * k_ref[u].astype(jnp.float32), axis=-1, keepdims=True) for u in range(t + 1)
        ]
        peak = functools.reduce(jnp.maximum, scores)
        weights = [jnp.exp(s - peak) for s in scores]
        total = functools.reduce(jnp.add, weights)
        accum = functools.reduce(
            jnp.add, [w * v_ref[u].astype(jnp.float32) for u, w in enumerate(weights)]
        )
        o_ref[t] = (accum / total).astype(o_ref.dtype)


def attend(query, keys, values):
    frames, rows, heads_width = query.shape
    heads = heads_width // HS
    spec = pl.BlockSpec((frames, rows, HS), lambda h: (0, 0, h))
    return pl.pallas_call(
        functools.partial(attend_kernel, frames),
        grid=(heads,),
        in_specs=[spec] * 3,
        out_specs=spec,
        out_shape=jax.ShapeDtypeStruct((frames, rows, heads_width), jnp.bfloat16),
        cost_estimate=pl.CostEstimate(flops=4 * frames * frames * rows * heads_width,
                                      bytes_accessed=8 * frames * rows * heads_width,
                                      transcendentals=0),
        name="attend",
    )(query, keys, values)


def spread_kernel(frames, dps, x_ref, o_ref, send_sem, recv_sem, own_sem):
    count = frames * dps
    me = lax.axis_index("frame") * dps + lax.axis_index("dp")
    barrier = pltpu.get_barrier_semaphore()

    def peer(shift):
        other = lax.rem(me + shift, count)
        return {"frame": other // dps, "dp": lax.rem(other, dps)}

    for shift in range(1, count):
        pl.semaphore_signal(barrier, inc=1, device_id=peer(shift),
                            device_id_type=pl.DeviceIdType.MESH)
    own = pltpu.make_async_copy(x_ref, o_ref.at[me], own_sem)
    own.start()
    pl.semaphore_wait(barrier, count - 1)
    copies = []
    for shift in range(1, count):
        copy = pltpu.make_async_remote_copy(
            src_ref=x_ref, dst_ref=o_ref.at[me], send_sem=send_sem.at[shift],
            recv_sem=recv_sem.at[shift], device_id=peer(shift),
            device_id_type=pl.DeviceIdType.MESH)
        copy.start()
        copies.append(copy)
    own.wait()
    for copy in copies:
        copy.wait()


def spread_terms(terms, frames, dps):
    count = frames * dps
    return pl.pallas_call(
        functools.partial(spread_kernel, frames, dps),
        in_specs=[pl.BlockSpec(memory_space=pltpu.VMEM)],
        out_specs=pl.BlockSpec(memory_space=pltpu.VMEM),
        out_shape=jax.ShapeDtypeStruct((count, *terms.shape), terms.dtype),
        scratch_shapes=[pltpu.SemaphoreType.DMA((count,)), pltpu.SemaphoreType.DMA((count,)),
                        pltpu.SemaphoreType.DMA],
        compiler_params=pltpu.CompilerParams(collective_id=1, has_side_effects=True),
        name="spread_terms",
    )(terms)


def return_kernel(frames, x_ref, mine_ref, other_ref, send_sem, recv_sem, fwd_send, fwd_recv,
                  own_sem):
    me = lax.axis_index("frame")
    across = {"mp": 1 - lax.axis_index("mp")}
    barrier = pltpu.get_barrier_semaphore()
    mesh_id = pl.DeviceIdType.MESH
    for shift in range(1, frames):
        pl.semaphore_signal(barrier, inc=1, device_id={"frame": lax.rem(me + shift, frames)},
                            device_id_type=mesh_id)
    pl.semaphore_signal(barrier, inc=1, device_id=across, device_id_type=mesh_id)
    own = pltpu.make_async_copy(x_ref.at[me], mine_ref.at[me], own_sem)
    own.start()
    pl.semaphore_wait(barrier, frames)
    copies = []
    for shift in range(1, frames):
        there = lax.rem(me + shift, frames)
        copy = pltpu.make_async_remote_copy(
            src_ref=x_ref.at[there], dst_ref=mine_ref.at[me], send_sem=send_sem.at[shift],
            recv_sem=recv_sem.at[shift], device_id={"frame": there}, device_id_type=mesh_id)
        copy.start()
        copies.append(copy)

    forwards = []
    for shift in range(frames):
        if shift:
            copies[shift - 1].wait_recv()
        else:
            own.wait()
        source = lax.rem(me - shift + frames, frames)
        copy = pltpu.make_async_remote_copy(
            src_ref=mine_ref.at[source], dst_ref=other_ref.at[source],
            send_sem=fwd_send.at[shift], recv_sem=fwd_recv.at[shift], device_id=across,
            device_id_type=mesh_id)
        copy.start()
        forwards.append(copy)
    for copy in copies:
        copy.wait_send()
    for copy in forwards:
        copy.wait()


def return_heads(attn):
    frames = attn.shape[0]
    out = jax.ShapeDtypeStruct(attn.shape, attn.dtype)
    return pl.pallas_call(
        functools.partial(return_kernel, frames),
        in_specs=[pl.BlockSpec(memory_space=pltpu.VMEM)],
        out_specs=[pl.BlockSpec(memory_space=pltpu.VMEM)] * 2,
        out_shape=[out, out],
        scratch_shapes=[pltpu.SemaphoreType.DMA((frames,))] * 4 + [pltpu.SemaphoreType.DMA],
        compiler_params=pltpu.CompilerParams(collective_id=2, has_side_effects=True),
        name="return_heads",
    )(attn)


def gather_mp(block, size):
    if size != 2:
        return lax.all_gather(block, "mp", axis=block.ndim - 1, tiled=True)
    other = lax.ppermute(block, "mp", [(0, 1), (1, 0)])
    first = lax.axis_index("mp") == 0
    return jnp.concatenate(
        [jnp.where(first, block, other), jnp.where(first, other, block)], axis=-1
    )


def body(mp_size, dp_size, tokens, token_mask, mask_embed, w_qkv, w_out, action_idx, codebook,
         act_proj, cotangent):
    clips, _, spots, width = tokens.shape
    heads_width = w_qkv.shape[2]
    depth = w_qkv.shape[0]
    xin = jnp.where(token_mask[..., None] == 1, mask_embed, tokens)
    share = depth // dp_size
    start = lax.axis_index("dp") * share
    weights = []
    for part in range(3):
        mine = lax.dynamic_slice(
            w_qkv, (start, part, 0), (share, 1, heads_width)).reshape(share, heads_width)
        if weights:
            mine, _ = lax.optimization_barrier((mine, weights[-1][:1, :1]))
        weights.append(lax.all_gather(mine, ("frame", "dp"), axis=0, tiled=True))
    if mp_size == 2:
        my_mp = lax.axis_index("mp")
        out_mine = lax.dynamic_slice_in_dim(w_out, my_mp * width, width, axis=1)
        out_other = lax.ppermute(
            lax.dynamic_slice_in_dim(w_out, (1 - my_mp) * width, width, axis=1),
            "mp", [(0, 1), (1, 0)])
    spread = lax.all_to_all(
        xin.reshape(clips, spots, width), "frame", split_axis=1, concat_axis=0, tiled=True
    )
    frames = spread.shape[0] // clips
    local = spread.shape[1]
    features = gather_mp(spread.reshape(frames * clips * local, width), mp_size)
    query, keys, values = [
        jnp.dot(features, w, preferred_element_type=jnp.float32)
        .astype(jnp.bfloat16)
        .reshape(frames, clips * local, heads_width)
        for w in weights
    ]
    attn = attend(query, keys, values)
    in_order = lambda blocks: (
        blocks.reshape(frames, clips, local, heads_width)
        .transpose(1, 0, 2, 3)
        .reshape(clips * spots, heads_width)
    )
    if mp_size == 2:
        heads, other_heads = [in_order(blocks) for blocks in return_heads(attn)]
        mixed_rows = jnp.dot(heads, out_mine, preferred_element_type=jnp.float32) + jnp.dot(
            other_heads, out_other, preferred_element_type=jnp.float32)
    else:
        heads = in_order(
            lax.all_to_all(attn, "frame", split_axis=0, concat_axis=0, tiled=True))
        out_block = lax.all_to_all(w_out, "mp", split_axis=1, concat_axis=0, tiled=True)
        mixed_rows = jnp.dot(gather_mp(heads, mp_size), out_block,
                             preferred_element_type=jnp.float32)
    mixed = mixed_rows.reshape(clips, 1, spots, width)
    onehot = (
        action_idx.reshape(clips)[:, None] == jnp.arange(codebook.shape[0])[None, :]
    ).astype(jnp.float32)
    codevec = jnp.dot(onehot, codebook, precision=lax.Precision.HIGHEST)
    gate = jnp.dot(codevec, act_proj, precision=lax.Precision.HIGHEST)
    next_state = (xin.astype(jnp.float32) + gate[:, None, None, :] * mixed).astype(jnp.bfloat16)
    dgate = jnp.sum(cotangent.astype(jnp.float32) * mixed, axis=2).reshape(clips, width)
    codes = codevec.shape[1]
    padded = jnp.pad(codevec, ((0, 0), (0, -codes % 128)))
    terms = spread_terms(jnp.concatenate([dgate, padded], axis=1), frames, dp_size)
    terms = terms.reshape(frames * dp_size * clips, -1)
    grad_proj = jnp.dot(
        terms[:, width : width + codes].T, terms[:, :width], precision=lax.Precision.HIGHEST)
    return (next_state, grad_proj)


def solution(mesh):
    in_specs = (
        P("dp", "frame", None, "mp"),
        P("dp", "frame", None),
        P("mp"),
        P("frame", None, "mp"),
        P("mp", None),
        P("dp", "frame"),
        P(),
        P(None, "mp"),
        P("dp", "frame", None, "mp"),
    )
    out_specs = (P("dp", "frame", None, "mp"), P(None, "mp"))
    return jax.shard_map(
        functools.partial(body, mesh.shape["mp"], mesh.shape["dp"]),
        mesh=mesh, in_specs=in_specs, out_specs=out_specs, check_vma=False,
    )
```
